128 devices in a mesh: sys: 1, aux: 16 (over z, y), orb: 8 (over x, core).
Axes of the slice: x: 4, y: 4, z: 4, core: 2. Of those that a mesh axis runs over, the one named last changes fastest.
Arguments:
- b_tensor: float32 [1152, 448, 448], P(('sys', 'aux'), 'orb')
- c_alpha: float32 [448, 39], P('sys')
- c_beta: float32 [448, 38], P('sys')
Outputs:
- output 1: float32 [448, 448], P(('sys', 'orb'), 'aux')
- output 2: float32 [448, 448], P(('sys', 'orb'), 'aux')
All inputs are finite; a program needn't handle non-finite values.
Results may differ from the reference program's by a relative error of at most 0.001.
Values are sent between devices in bfloat16 or wider.
A program may use at most 1 GiB of HBM per device.

```python
import math
import jax
import jax.numpy as jnp
from jax import lax

N = 448
NAUX = 1152
NALPHA = 39
NBETA = 38

TOP_PRECISION = lax.Precision.HIGHEST


def setup_inputs(seed: int = 0, part: int = 0) -> dict:
    pattern_count = 16
    root_key = jax.random.fold_in(jax.random.key(seed), part)
    key_noise, key_amp, key_orb, key_alpha, key_beta = jax.random.split(root_key, 5)
    amp_scale = (math.sqrt(pattern_count) / (NAUX * (NALPHA + NBETA))) ** 0.5
    raw_noise = jax.random.normal(key_noise, (NAUX, N, N), jnp.float32)
    sym_noise = (raw_noise + jnp.swapaxes(raw_noise, 1, 2)) * (0.5 * amp_scale / math.sqrt(2.0))
    amp_vals = jax.random.normal(key_amp, (NAUX,), jnp.float32) * amp_scale
    orb_pattern = jax.random.normal(key_orb, (pattern_count, N), jnp.float32)
    pattern_rows = jnp.repeat(orb_pattern, NAUX // pattern_count, axis=0)
    outer_prod = pattern_rows[:, :, None] * pattern_rows[:, None, :]
    b_tensor = sym_noise + amp_vals[:, None, None] * outer_prod
    c_alpha = jax.random.normal(key_alpha, (N, NALPHA), jnp.float32) / math.sqrt(N)
    c_beta = jax.random.normal(key_beta, (N, NBETA), jnp.float32) / math.sqrt(N)
    return {'b_tensor': b_tensor, 'c_alpha': c_alpha, 'c_beta': c_beta}


def reference(b_tensor, c_alpha, c_beta):
    b_full = b_tensor.astype(jnp.float32)
    alpha_full = c_alpha.astype(jnp.float32)
    beta_full = c_beta.astype(jnp.float32)
    dens_mat = jnp.dot(alpha_full, alpha_full.T, precision=TOP_PRECISION, preferred_element_type=jnp.float32) + jnp.dot(beta_full, beta_full.T, precision=TOP_PRECISION, preferred_element_type=jnp.float32)
    gamma_vec = jnp.einsum('qms,ms->q', b_full, dens_mat, precision=TOP_PRECISION)
    coul_mat = jnp.einsum('qmn,q->mn', b_full, gamma_vec, precision=TOP_PRECISION)

    def exchange(c_spin):
        half_tr = jnp.einsum('qml,li->qmi', b_full, c_spin, precision=TOP_PRECISION)
        return jnp.einsum('qmi,qni->mn', half_tr, half_tr, precision=TOP_PRECISION)

    return coul_mat - exchange(alpha_full), coul_mat - exchange(beta_full)
```

```python
import functools

import jax
import jax.numpy as jnp
from jax import lax
from jax.experimental import pallas as pl
from jax.experimental.pallas import tpu as pltpu
from jax.sharding import PartitionSpec as P

TOP_PRECISION = lax.Precision.HIGHEST
F32 = jnp.float32
MESH = pl.DeviceIdType.MESH

NX, NC = 4, 2
NZ, NY = 4, 4
NORB = NX * NC
PACK = 3
LANES = 128
SLOT = 64
HALF = 32


def dot(a, b):
    return jnp.dot(a, b, precision=TOP_PRECISION, preferred_element_type=F32)


def kernel(dims, b_hbm, cw_ref, oa_ref, ob_ref,
           bbuf, tsend, trecv, tlhs, pbuf, gsend, grecv, gam, jblk, kbuf,
           xrecv, s1, r1, s2, r2, s3, r3,
           b_sem, ts_sem, tr_sem, gs_sem, gr_sem, xs_sem, xr_sem,
           s1_sem, r1_sem, s2_sem, r2_sem, s3_sem, r3_sem):
    ng, ml, nbas, na, nb = dims
    gpc = NC * ng
    aux = lax.axis_index("aux")
    me = lax.axis_index("orb")
    sysi = lax.axis_index("sys")
    xi, hi = me // NC, me % NC
    zi, yi = aux // NY, aux % NY
    partner = me + 1 - 2 * hi
    p_idx = jnp.where(hi == 0, zi, yi)
    s_idx = jnp.where(hi == 0, yi, zi)
    p_stride = jnp.where(hi == 0, NY, 1)
    s_stride = jnp.where(hi == 0, 1, NY)

    def first_peer(d):
        q = (p_idx + d) % NZ
        return q, (sysi, q * p_stride + s_idx * s_stride, me)

    def second_peer(d):
        q = (s_idx + d) % NZ
        return q, (sysi, p_idx * p_stride + q * s_stride, me)

    def orb_dev(o):
        return (sysi, aux, o)

    def b_copy(i, xp):
        return pltpu.make_async_copy(b_hbm.at[pl.ds(xp * gpc, gpc)],
                                     bbuf.at[pl.ds(xp * gpc, gpc)], b_sem.at[i])

    def chunk_chip(i):
        off = jnp.where(i == 0, 2, jnp.where(i == 1, 1, jnp.where(i == 2, 3, 0)))
        return (xi + off) % NX

    for i in range(NX):
        b_copy(i, chunk_chip(i)).start()

    barrier = pltpu.get_barrier_semaphore()
    for o in range(1, NORB):
        pl.semaphore_signal(barrier, inc=1, device_id=orb_dev((me + o) % NORB), device_id_type=MESH)
    for d in range(1, NZ):
        pl.semaphore_signal(barrier, inc=1, device_id=first_peer(d)[1], device_id_type=MESH)
        pl.semaphore_signal(barrier, inc=1, device_id=second_peer(d)[1], device_id_type=MESH)

    for sp in range(2):
        for s in range(NORB):
            trecv[sp, s * SLOT + ml:(s + 1) * SLOT, :] = jnp.zeros((SLOT - ml, ng * LANES), F32)

    def t_copy(sp, dest, src):
        return pltpu.make_async_remote_copy(
            src_ref=tsend.at[sp, dest], dst_ref=trecv.at[sp, pl.ds(pl.multiple_of(src * SLOT, SLOT), ml)],
            send_sem=ts_sem.at[sp, dest], recv_sem=tr_sem.at[sp, src],
            device_id=orb_dev(dest), device_id_type=MESH)

    row0 = pl.multiple_of(me * ml, 8)
    crow = sum(cw_ref[j, pl.ds(row0, ml), :] for j in range(PACK))

    def t_chunk(i, _):
        xp = chunk_chip(i)
        b_copy(i, xp).wait()
        acc = None
        for j in range(PACK):
            lhs = bbuf[pl.ds(xp * gpc, gpc), j].reshape(gpc * ml, nbas)
            part = dot(lhs, cw_ref[j])
            acc = part if acc is None else acc + part
        for hh in range(NC):
            for g in range(ng):
                k = hh * ng + g
                blk = acc[k * ml:(k + 1) * ml]
                tsend[0, NC * xp + hh, :, g * LANES:(g + 1) * LANES] = blk[:, :LANES]
                tsend[1, NC * xp + hh, :, g * LANES:(g + 1) * LANES] = blk[:, LANES:]
                pbuf[pl.ds(xp * gpc + k, 1), :] = jnp.sum(blk * crow, axis=0, keepdims=True)

        @pl.when(i == 0)
        def _():
            pl.semaphore_wait(barrier, NORB - 1 + 2 * (NZ - 1))

        for hh in range(NC):
            dest = NC * xp + hh

            @pl.when(dest != me)
            def _():
                t_copy(0, dest, me).start()
        return 0

    lax.fori_loop(0, NX, t_chunk, 0)

    ngrp = NX * gpc
    nrow = ngrp // 8
    lane_i = lax.broadcasted_iota(jnp.int32, (2 * LANES, LANES), 0)
    lane_o = lax.broadcasted_iota(jnp.int32, (2 * LANES, LANES), 1)
    seg = jnp.where(lane_i < LANES, lane_i // na, (lane_i - LANES) // nb)
    seg = jnp.where(seg < PACK, seg, -LANES)
    gpart = jnp.zeros((8, LANES), F32)
    for r in range(nrow):
        sel = jnp.where(seg + PACK * r == lane_o, 1.0, 0.0).astype(F32)
        gpart = gpart + dot(pbuf[8 * r:8 * r + 8, :], sel)
    gsend[...] = gpart

    def g_copy(dest, src):
        return pltpu.make_async_remote_copy(
            src_ref=gsend, dst_ref=grecv.at[src], send_sem=gs_sem.at[dest], recv_sem=gr_sem.at[src],
            device_id=orb_dev(dest), device_id_type=MESH)

    for o in range(1, NORB):
        g_copy((me + o) % NORB, me).start()
    grecv[me] = gpart
    for i in range(NX):
        xp = chunk_chip(i)
        for hh in range(NC):
            dest = NC * xp + hh
            if i < NX - 1:
                t_copy(1, dest, me).start()
            else:
                @pl.when(dest != me)
                def _():
                    t_copy(1, dest, me).start()
    for sp in range(2):
        trecv[sp, pl.ds(pl.multiple_of(me * SLOT, SLOT), ml), :] = tsend[sp, me]

    def x_copy(sp):
        keep = pl.multiple_of(16 - 16 * hi, 16)
        return pltpu.make_async_remote_copy(
            src_ref=kbuf.at[sp, :, pl.ds(keep, 16)], dst_ref=xrecv.at[sp],
            send_sem=xs_sem.at[sp], recv_sem=xr_sem.at[sp],
            device_id=orb_dev(partner), device_id_type=MESH)

    def p1_copy(sp, d):
        q, dev = first_peer(d)
        return pltpu.make_async_remote_copy(
            src_ref=s1.at[sp, q], dst_ref=r1.at[sp, d - 1], send_sem=s1_sem.at[sp, d - 1],
            recv_sem=r1_sem.at[sp, d - 1], device_id=dev, device_id_type=MESH)

    def p2_copy(sp, d):
        q, dev = second_peer(d)
        return pltpu.make_async_remote_copy(
            src_ref=s2.at[sp, q], dst_ref=r2.at[sp, d - 1], send_sem=s2_sem.at[sp, d - 1],
            recv_sem=r2_sem.at[sp, d - 1], device_id=dev, device_id_type=MESH)

    def p3_copy(sp, dest, src):
        return pltpu.make_async_remote_copy(
            src_ref=s3.at[sp, dest // NC], dst_ref=r3.at[sp, src], send_sem=s3_sem.at[sp, dest],
            recv_sem=r3_sem.at[sp, src], device_id=orb_dev(dest), device_id_type=MESH)

    def exchange(sp):
        for o in range(1, NORB):
            src = (me + o) % NORB
            t_copy(sp, src, src).wait_recv()
        for s in range(NORB):
            base = s * SLOT
            tlhs[base:base + HALF, :] = trecv[sp, base:base + HALF, :]
            tlhs[base + HALF:base + SLOT, :] = trecv[sp, base + ml // 2:base + ml // 2 + HALF, :]
        nt = (((1,), (1,)), ((), ()))

        def rows(c, _):
            r0 = pl.multiple_of(c * 256, 256)
            prod = lax.dot_general(tlhs[pl.ds(r0, 256), :], trecv[sp], nt,
                                   precision=TOP_PRECISION, preferred_element_type=F32)
            kbuf[sp, pl.ds(c * 8, 8)] = (-prod).reshape(8, HALF, NORB * SLOT)
            return 0

        lax.fori_loop(0, 2, rows, 0)

    def coulomb():
        for o in range(1, NORB):
            src = (me + o) % NORB
            g_copy(src, src).wait_recv()
        gsum = grecv[0]
        for s in range(1, NORB):
            gsum = gsum + grecv[s]
        for r in range(nrow):
            for j in range(PACK):
                c = PACK * r + j
                gam[c * 8:c * 8 + 8, :] = jnp.broadcast_to(gsum[:, c:c + 1], (8, LANES))

        def add(g, acc):
            r, row = g // 8, g % 8
            for j in range(PACK):
                w = gam[pl.ds((PACK * r + j) * 8 + row, 1), :][:, :1]
                acc = acc + bbuf[g, j] * w
            return acc

        jmat = lax.fori_loop(0, ngrp, add, jnp.zeros((ml, nbas), F32))
        col = lax.broadcasted_iota(jnp.int32, (nbas, NORB * SLOT), 0)
        lane = lax.broadcasted_iota(jnp.int32, (nbas, NORB * SLOT), 1)
        spread = jnp.where((col // ml) * SLOT + col % ml == lane, 1.0, 0.0).astype(F32)
        jblk[...] = dot(jmat, spread)

    def add_coulomb(sp):
        half = ml // 2
        kbuf[sp, 2 * me, 0:half, :] = kbuf[sp, 2 * me, 0:half, :] + jblk[0:half, :]
        kbuf[sp, 2 * me + 1, 0:half, :] = kbuf[sp, 2 * me + 1, 0:half, :] + jblk[half:ml, :]
        x_copy(sp).start()

    def stage1(sp):
        x_copy(sp).wait_recv()
        mine = pl.multiple_of(16 * hi, 16)
        for p in range(NZ):
            for s in range(NY):
                slot = jnp.where(hi == 0, NY * p + s, NY * s + p)
                s1[sp, p, s] = kbuf[sp, slot, pl.ds(mine, 16), :] + xrecv[sp, slot]
        for d in (2, 1, 3):
            p1_copy(sp, d).start()

    def stage2(sp):
        for d in (1, 3, 2):
            p1_copy(sp, d).wait_recv()
        s2[sp] = ((s1[sp, p_idx] + r1[sp, 0]) + r1[sp, 1]) + r1[sp, 2]
        for d in (2, 1, 3):
            p2_copy(sp, d).start()

    def stage3(sp):
        for d in (1, 3, 2):
            p2_copy(sp, d).wait_recv()
        tot = ((s2[sp, s_idx] + r2[sp, 0]) + r2[sp, 1]) + r2[sp, 2]
        for x in range(NX):
            s3[sp, x] = tot[:, x * LANES:(x + 1) * LANES]
        for o in range(1, NORB):
            p3_copy(sp, (me + o) % NORB, me).start()
        r3[sp, me] = s3[sp, xi]

    def finish(sp, o_ref):
        for o in range(1, NORB):
            src = (me + o) % NORB
            p3_copy(sp, src, src).wait_recv()
        for h in range(NC):
            tot = r3[sp, h]
            for x in range(1, NX):
                tot = tot + r3[sp, NC * x + h]
            o_ref[16 * h:16 * h + 16, :] = tot

    exchange(0)
    coulomb()
    add_coulomb(0)
    stage1(0)
    exchange(1)
    add_coulomb(1)
    stage2(0)
    stage1(1)
    stage3(0)
    stage2(1)
    stage3(1)
    finish(0, oa_ref)
    finish(1, ob_ref)

    for sp in range(2):
        for o in range(1, NORB):
            dest = (me + o) % NORB
            t_copy(sp, dest, me).wait_send()
            p3_copy(sp, dest, me).wait_send()
        x_copy(sp).wait_send()
        for d in range(1, NZ):
            p1_copy(sp, d).wait_send()
            p2_copy(sp, d).wait_send()
    for o in range(1, NORB):
        g_copy((me + o) % NORB, me).wait_send()


def solution(mesh):
    def local_build(b_local, c_alpha, c_beta):
        q_loc, ml, nbas = b_local.shape
        na, nb = c_alpha.shape[1], c_beta.shape[1]
        ng = q_loc // (PACK * NORB)
        packed = []
        for j in range(PACK):
            packed.append(jnp.concatenate([
                jnp.pad(c_alpha, ((0, 0), (na * j, LANES - na * (j + 1)))),
                jnp.pad(c_beta, ((0, 0), (nb * j, LANES - nb * (j + 1))))], axis=1))
        cw = jnp.stack(packed)
        b4 = b_local.reshape(q_loc // PACK, PACK, ml, nbas)
        lanes = ng * LANES
        width = NORB * SLOT
        dma = pltpu.SemaphoreType.DMA
        out = pl.pallas_call(
            functools.partial(kernel, (ng, ml, nbas, na, nb)),
            out_shape=[jax.ShapeDtypeStruct((HALF, LANES), F32)] * 2,
            in_specs=[pl.BlockSpec(memory_space=pl.ANY), pl.BlockSpec(memory_space=pltpu.VMEM)],
            out_specs=[pl.BlockSpec(memory_space=pltpu.VMEM)] * 2,
            scratch_shapes=[
                pltpu.VMEM(b4.shape, F32),
                pltpu.VMEM((2, NORB, ml, lanes), F32),
                pltpu.VMEM((2, width, lanes), F32),
                pltpu.VMEM((width, lanes), F32),
                pltpu.VMEM((q_loc // PACK, 2 * LANES), F32),
                pltpu.VMEM((8, LANES), F32),
                pltpu.VMEM((NORB, 8, LANES), F32),
                pltpu.VMEM((q_loc, LANES), F32),
                pltpu.VMEM((ml, width), F32),
                pltpu.VMEM((2, NZ * NY, HALF, width), F32),
                pltpu.VMEM((2, NZ * NY, HALF // 2, width), F32),
                pltpu.VMEM((2, NZ, NY, HALF // 2, width), F32),
                pltpu.VMEM((2, NZ - 1, NY, HALF // 2, width), F32),
                pltpu.VMEM((2, NY, HALF // 2, width), F32),
                pltpu.VMEM((2, NZ - 1, HALF // 2, width), F32),
                pltpu.VMEM((2, NX, HALF // 2, LANES), F32),
                pltpu.VMEM((2, NORB, HALF // 2, LANES), F32),
                dma((NX,)), dma((2, NORB)), dma((2, NORB)), dma((NORB,)), dma((NORB,)),
                dma((2,)), dma((2,)),
                dma((2, NZ - 1)), dma((2, NZ - 1)), dma((2, NZ - 1)), dma((2, NZ - 1)),
                dma((2, NORB)), dma((2, NORB)),
            ],
            compiler_params=pltpu.CompilerParams(
                collective_id=0, has_side_effects=True, vmem_limit_bytes=60 * 1024 * 1024),
        )(b4, cw)
        core = lax.axis_index("orb") % NC
        n_aux_cols = nbas // (NZ * NY)

        def place(block):
            half = jnp.where(core == 0, block[:, :SLOT], block[:, SLOT:])
            return half[:n_aux_cols, :ml].T

        return place(out[0]), place(out[1])

    spec_b = P(('sys', 'aux'), 'orb', None)
    spec_c = P('sys', None)
    spec_g = P(('sys', 'orb'), 'aux')
    return jax.shard_map(local_build, mesh=mesh, in_specs=(spec_b, spec_c, spec_c), out_specs=(spec_g, spec_g), check_vma=False)
```

```python
import functools

import jax
import jax.numpy as jnp
from jax import lax
from jax.experimental import pallas as pl
from jax.experimental.pallas import tpu as pltpu
from jax.sharding import PartitionSpec as P

TOP_PRECISION = lax.Precision.HIGHEST
F32 = jnp.float32
MESH = pl.DeviceIdType.MESH

NX, NC = 4, 2
NZ, NY = 4, 4
NORB = NX * NC
PACK = 3
LANES = 128
SLOT = 64
HALF = 32
WIDE = NORB * SLOT // NC
NT = (((1,), (1,)), ((), ()))


def dot(a, b):
    return jnp.dot(a, b, precision=TOP_PRECISION, preferred_element_type=F32)


def dot_nt(a, b):
    return lax.dot_general(a, b, NT, precision=TOP_PRECISION, preferred_element_type=F32)


def iota(shape, dim):
    return lax.broadcasted_iota(jnp.int32, shape, dim)


def kernel(dims, b_hbm, ca_ref, cb_ref, oa_ref, ob_ref,
           bbuf, cwt, tsend, rel, trecv, tlhs, pbuf, gsend, grecv, gam, jown, jother, jfull,
           kbuf, r1, s2, r2, s3, r3,
           b_sem, ts_sem, tr_sem, rr_sem, rs_sem, ps_sem, pr_sem, gs_sem, gr_sem, j_sem,
           s1_sem, r1_sem, s2_sem, r2_sem, s3_sem, r3_sem):
    ng, ml, nbas, na, nb = dims
    gpc = NC * ng
    lanes = ng * LANES
    cols = nbas // (NZ * NY)
    aux = lax.axis_index("aux")
    me = lax.axis_index("orb")
    sysi = lax.axis_index("sys")
    xi, hi = me // NC, me % NC
    zi, yi = aux // NY, aux % NY
    partner = me + 1 - 2 * hi
    step = 1 + 2 * hi
    p_idx = jnp.where(hi == 0, zi, yi)
    s_idx = jnp.where(hi == 0, yi, zi)
    p_stride = jnp.where(hi == 0, NY, 1)
    s_stride = jnp.where(hi == 0, 1, NY)

    def first_peer(d):
        q = (p_idx + d) % NZ
        return q, (sysi, q * p_stride + s_idx * s_stride, me)

    def second_peer(d):
        q = (s_idx + d) % NZ
        return q, (sysi, p_idx * p_stride + q * s_stride, me)

    def orb_dev(o):
        return (sysi, aux, o)

    def remote(src, dst, send, recv, dev):
        return pltpu.make_async_remote_copy(src_ref=src, dst_ref=dst, send_sem=send, recv_sem=recv,
                                            device_id=dev, device_id_type=MESH)

    def b_copy(i, xp):
        return pltpu.make_async_copy(b_hbm.at[pl.ds(xp * gpc, gpc)],
                                     bbuf.at[pl.ds(xp * gpc, gpc)], b_sem.at[i])

    def chunk_chip(i):
        near = jnp.where(i == 1, step, NX - step)
        off = jnp.where(i == 0, 2, jnp.where(i == NX - 1, 0, near))
        return (xi + off) % NX

    for i in range(NX):
        b_copy(i, chunk_chip(i)).start()

    barrier = pltpu.get_barrier_semaphore()
    for o in range(1, NORB):
        pl.semaphore_signal(barrier, inc=1, device_id=orb_dev((me + o) % NORB), device_id_type=MESH)
    for d in range(1, NZ):
        pl.semaphore_signal(barrier, inc=1, device_id=first_peer(d)[1], device_id_type=MESH)
        pl.semaphore_signal(barrier, inc=1, device_id=second_peer(d)[1], device_id_type=MESH)

    for j in range(PACK):
        cwt[j] = jnp.zeros((2 * LANES, nbas), F32)
        cwt[j, na * j:na * (j + 1), :] = ca_ref[...]
        cwt[j, LANES + nb * j:LANES + nb * (j + 1), :] = cb_ref[...]
    for sp in range(2):
        for s in range(NORB):
            trecv[sp, s * SLOT + ml:(s + 1) * SLOT, :] = jnp.zeros((SLOT - ml, NC * lanes), F32)
        for s in range(NY):
            s2[sp, s, HALF - 8:HALF, :] = jnp.zeros((8, WIDE), F32)
    rowsel = jnp.where(iota((ml, nbas), 1) == me * ml + iota((ml, nbas), 0), 1.0, 0.0).astype(F32)
    crow = dot_nt(rowsel, cwt[0] + cwt[1] + cwt[2])

    def rows_of(src):
        return pl.ds(pl.multiple_of(src * SLOT, SLOT), ml)

    def t_copy(sp, dest, src):
        return remote(tsend.at[sp, dest], trecv.at[sp, rows_of(src), pl.ds(0, lanes)],
                      ts_sem.at[sp, dest], tr_sem.at[sp, src], orb_dev(dest))

    def relay_in(sp, hh):
        dest = NC * ((xi + 2) % NX) + hh
        return remote(tsend.at[sp, dest], rel.at[sp, hh], ts_sem.at[sp, dest], rr_sem.at[sp, hh],
                      orb_dev(NC * ((xi + step) % NX) + hi))

    def relay_out(sp, hh):
        src = NC * ((xi + NX - step) % NX) + hi
        return remote(rel.at[sp, hh], trecv.at[sp, rows_of(src), pl.ds(0, lanes)],
                      rs_sem.at[sp, hh], tr_sem.at[sp, src], orb_dev(NC * ((xi + step) % NX) + hh))

    def share(sp, src):
        return remote(trecv.at[sp, rows_of(src), pl.ds(0, lanes)],
                      trecv.at[sp, rows_of(src), pl.ds(lanes, lanes)],
                      ps_sem.at[sp, src], pr_sem.at[sp, src], orb_dev(partner))

    def share_own(sp):
        return remote(tsend.at[sp, me], trecv.at[sp, rows_of(me), pl.ds(lanes, lanes)],
                      ps_sem.at[sp, me], pr_sem.at[sp, me], orb_dev(partner))

    def t_chunk(i, _):
        xp = chunk_chip(i)
        b_copy(i, xp).wait()
        acc = None
        for j in range(PACK):
            lhs = bbuf[pl.ds(xp * gpc, gpc), j].reshape(gpc * ml, nbas)
            part = dot_nt(lhs, cwt[j])
            acc = part if acc is None else acc + part
        for hh in range(NC):
            for g in range(ng):
                k = hh * ng + g
                blk = acc[k * ml:(k + 1) * ml]
                tsend[0, NC * xp + hh, :, g * LANES:(g + 1) * LANES] = blk[:, :LANES]
                tsend[1, NC * xp + hh, :, g * LANES:(g + 1) * LANES] = blk[:, LANES:]
                pbuf[pl.ds(xp * gpc + k, 1), :] = jnp.sum(blk * crow, axis=0, keepdims=True)

        @pl.when(i == 0)
        def _():
            pl.semaphore_wait(barrier, NORB - 1 + 2 * (NZ - 1))
            for sp in range(2):
                for hh in range(NC):
                    relay_in(sp, hh).start()

        @pl.when((i == 1) | (i == 2))
        def _():
            for hh in range(NC):
                t_copy(0, NC * xp + hh, me).start()

        @pl.when(i == NX - 1)
        def _():
            t_copy(0, partner, me).start()
            share_own(0).start()
        return 0

    lax.fori_loop(0, NX, t_chunk, 0)

    for hh in range(NC):
        relay_in(0, hh).wait_recv()
        relay_out(0, hh).start()

    ngrp = NX * gpc
    nrow = ngrp // 8
    lane_i = iota((2 * LANES, LANES), 0)
    lane_o = iota((2 * LANES, LANES), 1)
    seg = jnp.where(lane_i < LANES, lane_i // na, (lane_i - LANES) // nb)
    seg = jnp.where(seg < PACK, seg, -LANES)
    gpart = jnp.zeros((8, LANES), F32)
    for r in range(nrow):
        sel = jnp.where(seg + PACK * r == lane_o, 1.0, 0.0).astype(F32)
        gpart = gpart + dot(pbuf[8 * r:8 * r + 8, :], sel)
    gsend[...] = gpart

    def g_copy(dest, src):
        return remote(gsend, grecv.at[src], gs_sem.at[dest], gr_sem.at[src], orb_dev(dest))

    for o in range(1, NORB):
        g_copy((me + o) % NORB, me).start()
    grecv[me] = gpart
    near = [NC * chunk_chip(i) + hh for i in (1, 2) for hh in range(NC)]
    far = [NC * ((xi + 2) % NX) + hh for hh in range(NC)]
    for dest in near:
        t_copy(1, dest, me).start()
    t_copy(1, partner, me).start()
    share_own(1).start()
    for sp in range(2):
        trecv[sp, rows_of(me), 0:lanes] = tsend[sp, me]
        trecv[sp, rows_of(me), lanes:2 * lanes] = tsend[sp, partner]

    def pass_on(sp, sources):
        for src in sources:
            t_copy(sp, src, src).wait_recv()
            share(sp, src).start()

    def j_copy():
        return remote(jown.at[1 - hi], jother, j_sem.at[0], j_sem.at[1], orb_dev(partner))

    def p1_copy(sp, d):
        q, dev = first_peer(d)
        return remote(kbuf.at[sp, q], r1.at[sp, d - 1], s1_sem.at[sp, d - 1], r1_sem.at[sp, d - 1], dev)

    def p2_copy(sp, d):
        q, dev = second_peer(d)
        return remote(s2.at[sp, q], r2.at[sp, d - 1], s2_sem.at[sp, d - 1], r2_sem.at[sp, d - 1], dev)

    def p3_copy(sp, k):
        return remote(s3.at[sp, k // NC], r3.at[sp, xi], s3_sem.at[sp, k], r3_sem.at[sp, xi],
                      orb_dev(NX * hi + k))

    def p3_wait(sp, x):
        return remote(s3.at[sp, 0], r3.at[sp, x], s3_sem.at[sp, 0], r3_sem.at[sp, x],
                      orb_dev(NC * x + xi // NC))

    def coulomb():
        for o in range(1, NORB):
            src = (me + o) % NORB
            g_copy(src, src).wait_recv()
        gsum = grecv[0]
        for s in range(1, NORB):
            gsum = gsum + grecv[s]
        for r in range(nrow):
            for j in range(PACK):
                c = PACK * r + j
                gam[c * 8:c * 8 + 8, :] = jnp.broadcast_to(gsum[:, c:c + 1], (8, LANES))

        def add(g, acc):
            r, row = g // 8, g % 8
            for j in range(PACK):
                w = gam[pl.ds((PACK * r + j) * 8 + row, 1), :][:, :1]
                acc = acc + bbuf[g, j] * w
            return acc

        jmat = lax.fori_loop(0, ngrp, add, jnp.zeros((ml, nbas), F32))
        col = iota((nbas, NORB * SLOT), 0)
        spread = jnp.where((col // ml) * SLOT + col % ml == iota((nbas, NORB * SLOT), 1), 1.0, 0.0).astype(F32)
        wide = dot(jmat, spread)
        for h in range(NC):
            jown[h] = wide[:, h * WIDE:(h + 1) * WIDE]
        j_copy().start()
        row, r = iota((nbas, ml), 0), iota((nbas, ml), 1)
        pos = row // cols
        nat = jnp.where(hi == 0, pos, (pos % NZ) * NY + pos // NZ) * cols + row % cols
        own = jnp.where(nat == me * ml + r, 1.0, 0.0).astype(F32)
        other = jnp.where(nat == partner * ml + r, 1.0, 0.0).astype(F32)
        mine = dot(own, jown[hi])
        j_copy().wait_recv()
        jfull[...] = (mine + dot(other, jother[...])).reshape(NZ, NY * cols, WIDE)

    def exchange(sp):
        for o in range(1, NORB):
            share(sp, (me + o) % NORB).wait_recv()
        for h in range(NC):
            @pl.when(hi == h)
            def _():
                for a in range(NZ * NY):
                    at = a if h == 0 else (a % NY) * NZ + a // NY
                    base = (a // 2) * SLOT + (a % 2) * cols
                    tlhs[at * cols:(at + 1) * cols, :] = trecv[sp, base:base + cols, :]
        rhs = pl.ds(pl.multiple_of(WIDE * hi, WIDE), WIDE)

        def rows(c, _):
            r0 = pl.multiple_of(c * (2 * NY * cols), 8)
            prod = dot_nt(tlhs[pl.ds(r0, 2 * NY * cols), :], trecv[sp, rhs, :])
            kbuf[sp, pl.ds(2 * c, 2)] = jfull[pl.ds(2 * c, 2)] - prod.reshape(2, NY * cols, WIDE)
            return 0

        lax.fori_loop(0, NZ // 2, rows, 0)
        for d in (2, 1, 3):
            p1_copy(sp, d).start()

    def stage2(sp):
        for d in (1, 3, 2):
            p1_copy(sp, d).wait_recv()
        tot = ((kbuf[sp, p_idx] + r1[sp, 0]) + r1[sp, 1]) + r1[sp, 2]
        for s in range(NY):
            s2[sp, s, 0:cols, :] = tot[s * cols:(s + 1) * cols]
        for d in (2, 1, 3):
            p2_copy(sp, d).start()

    def stage3(sp):
        for d in (1, 3, 2):
            p2_copy(sp, d).wait_recv()
        tot = ((s2[sp, s_idx] + r2[sp, 0]) + r2[sp, 1]) + r2[sp, 2]
        for x in range(NX // NC):
            s3[sp, x] = tot[:, x * LANES:(x + 1) * LANES]
        for k in range(NX):
            @pl.when(NX * hi + k != me)
            def _():
                p3_copy(sp, k).start()

            @pl.when(NX * hi + k == me)
            def _():
                r3[sp, xi] = s3[sp, k // NC]

    def finish(sp, o_ref):
        for x in range(NX):
            @pl.when(NC * x + xi // NC != me)
            def _():
                p3_wait(sp, x).wait_recv()
        tot = ((r3[sp, 0] + r3[sp, 1]) + r3[sp, 2]) + r3[sp, 3]
        half = jnp.where(hi == 0, tot[:, :SLOT], tot[:, SLOT:])
        o_ref[...] = half[:cols, :ml]

    pass_on(0, near)
    for hh in range(NC):
        relay_in(1, hh).wait_recv()
        relay_out(1, hh).start()
    pass_on(0, far)
    t_copy(0, partner, partner).wait_recv()
    coulomb()
    exchange(0)
    pass_on(1, near)
    pass_on(1, far)
    t_copy(1, partner, partner).wait_recv()
    exchange(1)
    stage2(0)
    stage3(0)
    stage2(1)
    stage3(1)
    finish(0, oa_ref)
    finish(1, ob_ref)

    for sp in range(2):
        for dest in near + [partner]:
            t_copy(sp, dest, me).wait_send()
        for hh in range(NC):
            relay_in(sp, hh).wait_send()
            relay_out(sp, hh).wait_send()
        for src in near + far:
            share(sp, src).wait_send()
        share_own(sp).wait_send()
        for d in range(1, NZ):
            p1_copy(sp, d).wait_send()
            p2_copy(sp, d).wait_send()
        for k in range(NX):
            @pl.when(NX * hi + k != me)
            def _():
                p3_copy(sp, k).wait_send()
    for o in range(1, NORB):
        g_copy((me + o) % NORB, me).wait_send()
    j_copy().wait_send()


def solution(mesh):
    def local_build(b_local, c_alpha, c_beta):
        q_loc, ml, nbas = b_local.shape
        na, nb = c_alpha.shape[1], c_beta.shape[1]
        ng = q_loc // (PACK * NORB)
        b4 = b_local.reshape(q_loc // PACK, PACK, ml, nbas)
        lanes = ng * LANES
        width = NORB * SLOT
        cols = nbas // (NZ * NY)
        dma = pltpu.SemaphoreType.DMA
        vmem = pl.BlockSpec(memory_space=pltpu.VMEM)
        out = pl.pallas_call(
            functools.partial(kernel, (ng, ml, nbas, na, nb)),
            out_shape=[jax.ShapeDtypeStruct((cols, ml), F32)] * 2,
            in_specs=[pl.BlockSpec(memory_space=pl.ANY), vmem, vmem],
            out_specs=[vmem] * 2,
            scratch_shapes=[
                pltpu.VMEM(b4.shape, F32),
                pltpu.VMEM((PACK, 2 * LANES, nbas), F32),
                pltpu.VMEM((2, NORB, ml, lanes), F32),
                pltpu.VMEM((2, NC, ml, lanes), F32),
                pltpu.VMEM((2, width, NC * lanes), F32),
                pltpu.VMEM((nbas, NC * lanes), F32),
                pltpu.VMEM((q_loc // PACK, 2 * LANES), F32),
                pltpu.VMEM((8, LANES), F32),
                pltpu.VMEM((NORB, 8, LANES), F32),
                pltpu.VMEM((q_loc, LANES), F32),
                pltpu.VMEM((NC, ml, WIDE), F32),
                pltpu.VMEM((ml, WIDE), F32),
                pltpu.VMEM((NZ, NY * cols, WIDE), F32),
                pltpu.VMEM((2, NZ, NY * cols, WIDE), F32),
                pltpu.VMEM((2, NZ - 1, NY * cols, WIDE), F32),
                pltpu.VMEM((2, NY, HALF, WIDE), F32),
                pltpu.VMEM((2, NZ - 1, HALF, WIDE), F32),
                pltpu.VMEM((2, NX // NC, HALF, LANES), F32),
                pltpu.VMEM((2, NX, HALF, LANES), F32),
                dma((NX,)), dma((2, NORB)), dma((2, NORB)), dma((2, NC)), dma((2, NC)),
                dma((2, NORB)), dma((2, NORB)), dma((NORB,)), dma((NORB,)), dma((2,)),
                dma((2, NZ - 1)), dma((2, NZ - 1)), dma((2, NZ - 1)), dma((2, NZ - 1)),
                dma((2, NX)), dma((2, NX)),
            ],
            compiler_params=pltpu.CompilerParams(
                collective_id=0, has_side_effects=True, vmem_limit_bytes=60 * 1024 * 1024),
        )(b4, c_alpha.T, c_beta.T)
        return out[0].T, out[1].T

    spec_b = P(('sys', 'aux'), 'orb', None)
    spec_c = P('sys', None)
    spec_g = P(('sys', 'orb'), 'aux')
    return jax.shard_map(local_build, mesh=mesh, in_specs=(spec_b, spec_c, spec_c), out_specs=(spec_g, spec_g), check_vma=False)
```

```python
import functools

import jax
import jax.numpy as jnp
from jax import lax
from jax.experimental import pallas as pl
from jax.experimental.pallas import tpu as pltpu
from jax.sharding import PartitionSpec as P

TOP_PRECISION = lax.Precision.HIGHEST
F32 = jnp.float32
MESH = pl.DeviceIdType.MESH

NX, NC = 4, 2
NZ, NY = 4, 4
NORB = NX * NC
NAUX = NZ * NY
PACK = 3
LANES = 128
SLOT = 64
HALF = 32
WIDE = NORB * SLOT // NC
NT = (((1,), (1,)), ((), ()))


def dot(a, b):
    return jnp.dot(a, b, precision=TOP_PRECISION, preferred_element_type=F32)


def dot_nt(a, b):
    return lax.dot_general(a, b, NT, precision=TOP_PRECISION, preferred_element_type=F32)


def iota(shape, dim):
    return lax.broadcasted_iota(jnp.int32, shape, dim)


def kernel(dims, b_hbm, ca_ref, cb_ref, oa_ref, ob_ref,
           bbuf, cwt, tsend, trecv, tlhs, pbuf, gsend, grecv, gam, jpad, jsend, jrecv,
           kbuf, r1, s2, r2, s3, r3,
           b_sem, ts_sem, tr_sem, ps_sem, pr_sem, gs_sem, gr_sem, js_sem, jr_sem,
           s1_sem, r1_sem, s2_sem, r2_sem, s3_sem, r3_sem):
    ng, ml, nbas, na, nb = dims
    gpc = NC * ng
    lanes = ng * LANES
    cols = nbas // (NZ * NY)
    aux = lax.axis_index("aux")
    me = lax.axis_index("orb")
    sysi = lax.axis_index("sys")
    xi, hi = me // NC, me % NC
    zi, yi = aux // NY, aux % NY
    partner = me + 1 - 2 * hi
    step = 1 + 2 * hi
    p_idx = jnp.where(hi == 0, zi, yi)
    s_idx = jnp.where(hi == 0, yi, zi)
    p_stride = jnp.where(hi == 0, NY, 1)
    s_stride = jnp.where(hi == 0, 1, NY)

    def first_peer(d):
        q = (p_idx + d) % NZ
        return q, (sysi, q * p_stride + s_idx * s_stride, me)

    def second_peer(d):
        q = (s_idx + d) % NZ
        return q, (sysi, p_idx * p_stride + q * s_stride, me)

    def orb_dev(o):
        return (sysi, aux, o)

    def remote(src, dst, send, recv, dev):
        return pltpu.make_async_remote_copy(src_ref=src, dst_ref=dst, send_sem=send, recv_sem=recv,
                                            device_id=dev, device_id_type=MESH)

    def b_copy(i, xp):
        return pltpu.make_async_copy(b_hbm.at[pl.ds(xp * gpc, gpc)],
                                     bbuf.at[pl.ds(xp * gpc, gpc)], b_sem.at[i])

    def chunk_chip(i):
        near = jnp.where(i == 2, step, NX - step)
        off = jnp.where(i == 0, 2, jnp.where(i == 1, 0, near))
        return (xi + off) % NX

    for i in range(NX):
        b_copy(i, chunk_chip(i)).start()

    barrier = pltpu.get_barrier_semaphore()
    for o in range(1, NORB):
        pl.semaphore_signal(barrier, inc=1, device_id=orb_dev((me + o) % NORB), device_id_type=MESH)
    for k in range(1, NAUX):
        pl.semaphore_signal(barrier, inc=1, device_id=(sysi, (aux + k) % NAUX, me), device_id_type=MESH)

    for j in range(PACK):
        cwt[j] = jnp.zeros((2 * LANES, nbas), F32)
        cwt[j, na * j:na * (j + 1), :] = ca_ref[...]
        cwt[j, LANES + nb * j:LANES + nb * (j + 1), :] = cb_ref[...]
    for sp in range(2):
        for s in range(NORB):
            trecv[sp, s * SLOT + ml:(s + 1) * SLOT, :] = jnp.zeros((SLOT - ml, NC * lanes), F32)
        for s in range(NY):
            s2[sp, s, HALF - 8:HALF, :] = jnp.zeros((8, WIDE), F32)
    for a in range(NAUX):
        jsend[a, HALF - 8:HALF, :] = jnp.zeros((8, LANES), F32)
    jpad[...] = jnp.zeros(jpad.shape, F32)
    rowsel = jnp.where(iota((ml, nbas), 1) == me * ml + iota((ml, nbas), 0), 1.0, 0.0).astype(F32)
    crow = dot_nt(rowsel, cwt[0] + cwt[1] + cwt[2])

    def rows_of(src):
        return pl.ds(pl.multiple_of(src * SLOT, SLOT), ml)

    def t_copy(sp, dest, src):
        return remote(tsend.at[sp, dest], trecv.at[sp, rows_of(src), pl.ds(0, lanes)],
                      ts_sem.at[sp, dest], tr_sem.at[sp, src], orb_dev(dest))

    def share(sp, src):
        return remote(trecv.at[sp, rows_of(src), pl.ds(0, lanes)],
                      trecv.at[sp, rows_of(src), pl.ds(lanes, lanes)],
                      ps_sem.at[sp, src], pr_sem.at[sp, src], orb_dev(partner))

    def share_own(sp):
        return remote(tsend.at[sp, me], trecv.at[sp, rows_of(me), pl.ds(lanes, lanes)],
                      ps_sem.at[sp, me], pr_sem.at[sp, me], orb_dev(partner))

    def t_chunk(i, _):
        xp = chunk_chip(i)
        b_copy(i, xp).wait()
        acc = None
        for j in range(PACK):
            lhs = bbuf[pl.ds(xp * gpc, gpc), j].reshape(gpc * ml, nbas)
            part = dot_nt(lhs, cwt[j])
            acc = part if acc is None else acc + part
        for hh in range(NC):
            for g in range(ng):
                k = hh * ng + g
                blk = acc[k * ml:(k + 1) * ml]
                tsend[0, NC * xp + hh, :, g * LANES:(g + 1) * LANES] = blk[:, :LANES]
                tsend[1, NC * xp + hh, :, g * LANES:(g + 1) * LANES] = blk[:, LANES:]
                pbuf[pl.ds(xp * gpc + k, 1), :] = jnp.sum(blk * crow, axis=0, keepdims=True)

        @pl.when(i == 0)
        def _():
            pl.semaphore_wait(barrier, NORB - 1 + NAUX - 1)
            for sp in range(2):
                for hh in range(NC):
                    t_copy(sp, NC * xp + hh, me).start()

        @pl.when(i == 1)
        def _():
            for sp in range(2):
                t_copy(sp, partner, me).start()
                share_own(sp).start()

        @pl.when(i == 2)
        def _():
            for hh in range(NC):
                t_copy(0, NC * xp + hh, me).start()
        return 0

    lax.fori_loop(0, NX, t_chunk, 0)

    ngrp = NX * gpc
    nrow = ngrp // 8
    lane_i = iota((2 * LANES, LANES), 0)
    lane_o = iota((2 * LANES, LANES), 1)
    seg = jnp.where(lane_i < LANES, lane_i // na, (lane_i - LANES) // nb)
    seg = jnp.where(seg < PACK, seg, -LANES)
    gpart = jnp.zeros((8, LANES), F32)
    for r in range(nrow):
        sel = jnp.where(seg + PACK * r == lane_o, 1.0, 0.0).astype(F32)
        gpart = gpart + dot(pbuf[8 * r:8 * r + 8, :], sel)
    gsend[...] = gpart

    def g_copy(dest, src):
        return remote(gsend, grecv.at[src], gs_sem.at[dest], gr_sem.at[src], orb_dev(dest))

    for o in range(1, NORB):
        g_copy((me + o) % NORB, me).start()
    grecv[me] = gpart
    near = [NC * chunk_chip(i) + hh for i in (2, 3) for hh in range(NC)]
    far = [NC * chunk_chip(0) + hh for hh in range(NC)]
    for dest in near[2:]:
        t_copy(0, dest, me).start()
    for dest in near:
        t_copy(1, dest, me).start()
    for sp in range(2):
        trecv[sp, rows_of(me), 0:lanes] = tsend[sp, me]
        trecv[sp, rows_of(me), lanes:2 * lanes] = tsend[sp, partner]

    def pass_on(sp, sources):
        for src in sources:
            t_copy(sp, src, src).wait_recv()
            share(sp, src).start()

    def j_copy(dest, src):
        return remote(jsend.at[dest], jrecv.at[src], js_sem.at[dest], jr_sem.at[src], (sysi, dest, me))

    def p1_copy(sp, d):
        q, dev = first_peer(d)
        return remote(kbuf.at[sp, q], r1.at[sp, d - 1], s1_sem.at[sp, d - 1], r1_sem.at[sp, d - 1], dev)

    def p2_copy(sp, d):
        q, dev = second_peer(d)
        return remote(s2.at[sp, q], r2.at[sp, d - 1], s2_sem.at[sp, d - 1], r2_sem.at[sp, d - 1], dev)

    def p3_copy(sp, k):
        return remote(s3.at[sp, k // NC], r3.at[sp, xi], s3_sem.at[sp, k], r3_sem.at[sp, xi],
                      orb_dev(NX * hi + k))

    def p3_wait(sp, x):
        return remote(s3.at[sp, 0], r3.at[sp, x], s3_sem.at[sp, 0], r3_sem.at[sp, x],
                      orb_dev(NC * x + xi // NC))

    def coulomb():
        for o in range(1, NORB):
            src = (me + o) % NORB
            g_copy(src, src).wait_recv()
        gsum = grecv[0]
        for s in range(1, NORB):
            gsum = gsum + grecv[s]
        for r in range(nrow):
            for j in range(PACK):
                c = PACK * r + j
                gam[c * 8:c * 8 + 8, :] = jnp.broadcast_to(gsum[:, c:c + 1], (8, LANES))

        def add(g, acc):
            r, row = g // 8, g % 8
            for j in range(PACK):
                w = gam[pl.ds((PACK * r + j) * 8 + row, 1), :][:, :1]
                acc = acc + bbuf[g, j] * w
            return acc

        jmat = lax.fori_loop(0, ngrp, add, jnp.zeros((ml, nbas), F32))
        jpad[0:ml, 0:nbas] = jmat
        jt = jpad[...].T
        for a in range(NAUX):
            jsend[a, 0:cols, :] = jt[a * cols:(a + 1) * cols]
        for k in range(1, NAUX):
            j_copy((aux + k) % NAUX, aux).start()
        jrecv[aux] = jsend[aux]

    def exchange(sp):
        for o in range(1, NORB):
            share(sp, (me + o) % NORB).wait_recv()
        for h in range(NC):
            @pl.when(hi == h)
            def _():
                for a in range(NZ * NY):
                    at = a if h == 0 else (a % NY) * NZ + a // NY
                    base = (a // 2) * SLOT + (a % 2) * cols
                    tlhs[at * cols:(at + 1) * cols, :] = trecv[sp, base:base + cols, :]
        rhs = pl.ds(pl.multiple_of(WIDE * hi, WIDE), WIDE)

        def rows(c, _):
            r0 = pl.multiple_of(c * (2 * NY * cols), 8)
            prod = dot_nt(tlhs[pl.ds(r0, 2 * NY * cols), :], trecv[sp, rhs, :])
            kbuf[sp, pl.ds(2 * c, 2)] = prod.reshape(2, NY * cols, WIDE)
            return 0

        lax.fori_loop(0, NZ // 2, rows, 0)
        for d in (2, 1, 3):
            p1_copy(sp, d).start()

    def stage2(sp):
        for d in (1, 3, 2):
            p1_copy(sp, d).wait_recv()
        tot = ((kbuf[sp, p_idx] + r1[sp, 0]) + r1[sp, 1]) + r1[sp, 2]
        for s in range(NY):
            s2[sp, s, 0:cols, :] = tot[s * cols:(s + 1) * cols]
        for d in (2, 1, 3):
            p2_copy(sp, d).start()

    def stage3(sp):
        for d in (1, 3, 2):
            p2_copy(sp, d).wait_recv()
        tot = ((s2[sp, s_idx] + r2[sp, 0]) + r2[sp, 1]) + r2[sp, 2]
        for x in range(NX // NC):
            s3[sp, x] = tot[:, x * LANES:(x + 1) * LANES]
        for k in range(NX):
            @pl.when(NX * hi + k != me)
            def _():
                p3_copy(sp, k).start()

            @pl.when(NX * hi + k == me)
            def _():
                r3[sp, xi] = s3[sp, k // NC]

    def finish(sp, o_ref, jtot):
        for x in range(NX):
            @pl.when(NC * x + xi // NC != me)
            def _():
                p3_wait(sp, x).wait_recv()
        tot = ((r3[sp, 0] + r3[sp, 1]) + r3[sp, 2]) + r3[sp, 3]
        half = jnp.where(hi == 0, tot[:, :SLOT], tot[:, SLOT:])
        o_ref[...] = jtot[:cols, :ml] - half[:cols, :ml]

    pass_on(0, far)
    pass_on(1, far)
    for sp in range(2):
        t_copy(sp, partner, partner).wait_recv()
    coulomb()
    pass_on(0, near)
    exchange(0)
    pass_on(1, near)
    exchange(1)
    stage2(0)
    stage2(1)
    for k in range(1, NAUX):
        src = (aux + k) % NAUX
        j_copy(src, src).wait_recv()
    jtot = jrecv[0]
    for a in range(1, NAUX):
        jtot = jtot + jrecv[a]
    stage3(0)
    stage3(1)
    finish(0, oa_ref, jtot)
    finish(1, ob_ref, jtot)

    for sp in range(2):
        for dest in near + far + [partner]:
            t_copy(sp, dest, me).wait_send()
        for src in near + far:
            share(sp, src).wait_send()
        share_own(sp).wait_send()
        for d in range(1, NZ):
            p1_copy(sp, d).wait_send()
            p2_copy(sp, d).wait_send()
        for k in range(NX):
            @pl.when(NX * hi + k != me)
            def _():
                p3_copy(sp, k).wait_send()
    for o in range(1, NORB):
        g_copy((me + o) % NORB, me).wait_send()
    for k in range(1, NAUX):
        j_copy((aux + k) % NAUX, aux).wait_send()


def solution(mesh):
    def local_build(b_local, c_alpha, c_beta):
        q_loc, ml, nbas = b_local.shape
        na, nb = c_alpha.shape[1], c_beta.shape[1]
        ng = q_loc // (PACK * NORB)
        b4 = b_local.reshape(q_loc // PACK, PACK, ml, nbas)
        lanes = ng * LANES
        width = NORB * SLOT
        cols = nbas // (NZ * NY)
        dma = pltpu.SemaphoreType.DMA
        vmem = pl.BlockSpec(memory_space=pltpu.VMEM)
        out = pl.pallas_call(
            functools.partial(kernel, (ng, ml, nbas, na, nb)),
            out_shape=[jax.ShapeDtypeStruct((cols, ml), F32)] * 2,
            in_specs=[pl.BlockSpec(memory_space=pl.ANY), vmem, vmem],
            out_specs=[vmem] * 2,
            scratch_shapes=[
                pltpu.VMEM(b4.shape, F32),
                pltpu.VMEM((PACK, 2 * LANES, nbas), F32),
                pltpu.VMEM((2, NORB, ml, lanes), F32),
                pltpu.VMEM((2, width, NC * lanes), F32),
                pltpu.VMEM((nbas, NC * lanes), F32),
                pltpu.VMEM((q_loc // PACK, 2 * LANES), F32),
                pltpu.VMEM((8, LANES), F32),
                pltpu.VMEM((NORB, 8, LANES), F32),
                pltpu.VMEM((q_loc, LANES), F32),
                pltpu.VMEM((LANES, width), F32),
                pltpu.VMEM((NAUX, HALF, LANES), F32),
                pltpu.VMEM((NAUX, HALF, LANES), F32),
                pltpu.VMEM((2, NZ, NY * cols, WIDE), F32),
                pltpu.VMEM((2, NZ - 1, NY * cols, WIDE), F32),
                pltpu.VMEM((2, NY, HALF, WIDE), F32),
                pltpu.VMEM((2, NZ - 1, HALF, WIDE), F32),
                pltpu.VMEM((2, NX // NC, HALF, LANES), F32),
                pltpu.VMEM((2, NX, HALF, LANES), F32),
                dma((NX,)), dma((2, NORB)), dma((2, NORB)),
                dma((2, NORB)), dma((2, NORB)), dma((NORB,)), dma((NORB,)), dma((NAUX,)), dma((NAUX,)),
                dma((2, NZ - 1)), dma((2, NZ - 1)), dma((2, NZ - 1)), dma((2, NZ - 1)),
                dma((2, NX)), dma((2, NX)),
            ],
            compiler_params=pltpu.CompilerParams(
                collective_id=0, has_side_effects=True, vmem_limit_bytes=60 * 1024 * 1024),
        )(b4, c_alpha.T, c_beta.T)
        return out[0].T, out[1].T

    spec_b = P(('sys', 'aux'), 'orb', None)
    spec_c = P('sys', None)
    spec_g = P(('sys', 'orb'), 'aux')
    return jax.shard_map(local_build, mesh=mesh, in_specs=(spec_b, spec_c, spec_c), out_specs=(spec_g, spec_g), check_vma=False)
```

```python
import functools

import jax
import jax.numpy as jnp
from jax import lax
from jax.experimental import pallas as pl
from jax.experimental.pallas import tpu as pltpu
from jax.sharding import PartitionSpec as P

TOP_PRECISION = lax.Precision.HIGHEST
F32 = jnp.float32
MESH = pl.DeviceIdType.MESH

NX, NC = 4, 2
NZ, NY = 4, 4
NORB = NX * NC
NAUX = NZ * NY
PACK = 3
LANES = 128
SLOT = 64
HALF = 32
WIDE = NORB * SLOT // NC
NT = (((1,), (1,)), ((), ()))


def dot(a, b):
    return jnp.dot(a, b, precision=TOP_PRECISION, preferred_element_type=F32)


def dot_nt(a, b):
    return lax.dot_general(a, b, NT, precision=TOP_PRECISION, preferred_element_type=F32)


def iota(shape, dim):
    return lax.broadcasted_iota(jnp.int32, shape, dim)


def kernel(dims, b_hbm, ca_hbm, cb_hbm, o_ref,
           bbuf, ca_ref, cb_ref, cwt, tsend, trecv, tlhs, pbuf, gsend, grecv, gam, jpad, jsend, jrecv,
           kbuf, r1, s2, r2, s3, r3,
           b_sem, c_sem, ts_sem, tr_sem, ps_sem, pr_sem, gs_sem, gr_sem, js_sem, jr_sem,
           s1_sem, r1_sem, s2_sem, r2_sem, s3_sem, r3_sem):
    ng, ml, nbas, na, nb = dims
    cols = nbas // (NZ * NY)
    aux = lax.axis_index("aux")
    me = lax.axis_index("orb")
    sysi = lax.axis_index("sys")
    xi, hi = me // NC, me % NC
    zi, yi = aux // NY, aux % NY
    partner = me + 1 - 2 * hi
    step = 1 + 2 * hi
    p_idx = jnp.where(hi == 0, zi, yi)
    s_idx = jnp.where(hi == 0, yi, zi)
    p_stride = jnp.where(hi == 0, NY, 1)
    s_stride = jnp.where(hi == 0, 1, NY)

    def first_peer(d):
        q = (p_idx + d) % NZ
        return q, (sysi, q * p_stride + s_idx * s_stride, me)

    def second_peer(d):
        q = (s_idx + d) % NZ
        return q, (sysi, p_idx * p_stride + q * s_stride, me)

    def orb_dev(o):
        return (sysi, aux, o)

    def remote(src, dst, send, recv, dev):
        return pltpu.make_async_remote_copy(src_ref=src, dst_ref=dst, send_sem=send, recv_sem=recv,
                                            device_id=dev, device_id_type=MESH)

    gpc = NC * ng

    def chip_of(i):
        off = jnp.where(i == 0, 2, jnp.where(i == 1, step, jnp.where(i == 2, NX - step, 0)))
        return (xi + off) % NX

    far, side, back = ([NC * chip_of(i) + hh for hh in range(NC)] for i in range(3))
    near = side + back

    def b_copy(i):
        part = pl.ds(chip_of(i) * gpc, gpc)
        return pltpu.make_async_copy(b_hbm.at[part], bbuf.at[part], b_sem.at[i])

    b_copy(0).start()
    c_copies = [pltpu.make_async_copy(ca_hbm, ca_ref, c_sem.at[0]), pltpu.make_async_copy(cb_hbm, cb_ref, c_sem.at[1])]
    for c in c_copies:
        c.start()
    for i in range(1, NX):
        b_copy(i).start()

    barrier = pltpu.get_barrier_semaphore()
    for o in range(1, NORB):
        pl.semaphore_signal(barrier, inc=1, device_id=orb_dev((me + o) % NORB), device_id_type=MESH)
    for k in range(1, NAUX):
        pl.semaphore_signal(barrier, inc=1, device_id=(sysi, (aux + k) % NAUX, me), device_id_type=MESH)

    for sp in range(2):
        for g in range(ng):
            for s in range(NORB):
                trecv[sp, g, s * SLOT + ml:(s + 1) * SLOT, :] = jnp.zeros((SLOT - ml, NC * LANES), F32)
        for s in range(NY):
            s2[sp, s, HALF - 8:HALF, :] = jnp.zeros((8, WIDE), F32)
    for a in range(NAUX):
        jsend[a, HALF - 8:HALF, :] = jnp.zeros((8, LANES), F32)
    jpad[...] = jnp.zeros(jpad.shape, F32)
    for j in range(PACK):
        cwt[j] = jnp.zeros((2 * LANES, nbas), F32)
    for c in c_copies:
        c.wait()
    for j in range(PACK):
        cwt[j, na * j:na * (j + 1), :] = ca_ref[...]
        cwt[j, LANES + nb * j:LANES + nb * (j + 1), :] = cb_ref[...]
    rowsel = jnp.where(iota((ml, nbas), 1) == me * ml + iota((ml, nbas), 0), 1.0, 0.0).astype(F32)
    crow = dot_nt(rowsel, cwt[0] + cwt[1] + cwt[2])

    def rows_of(src):
        return pl.ds(pl.multiple_of(src * SLOT, SLOT), ml)

    def t_copy(sp, dest, src, g=None):
        part = pl.ds(0, ng) if g is None else g
        k = 0 if g is None else g
        return remote(tsend.at[sp, dest, part], trecv.at[sp, part, rows_of(src), pl.ds(0, LANES)],
                      ts_sem.at[sp, dest, k], tr_sem.at[sp, src, k], orb_dev(dest))

    def share(sp, src, g=None):
        part = pl.ds(0, ng) if g is None else g
        k = 0 if g is None else g
        return remote(trecv.at[sp, part, rows_of(src), pl.ds(0, LANES)],
                      trecv.at[sp, part, rows_of(src), pl.ds(LANES, LANES)],
                      ps_sem.at[sp, src, k], pr_sem.at[sp, src, k], orb_dev(partner))

    def share_own(sp):
        return remote(tsend.at[sp, me], trecv.at[sp, pl.ds(0, ng), rows_of(me), pl.ds(LANES, LANES)],
                      ps_sem.at[sp, me, 0], pr_sem.at[sp, me, 0], orb_dev(partner))

    def t_chunk(i, _):
        chip = chip_of(i)
        b_copy(i).wait()
        acc = None
        for j in range(PACK):
            part = dot_nt(bbuf[pl.ds(chip * gpc, gpc), j].reshape(gpc * ml, nbas), cwt[j])
            acc = part if acc is None else acc + part
        for k in range(gpc):
            blk = acc[k * ml:(k + 1) * ml]
            tsend[0, NC * chip + k // ng, k % ng] = blk[:, :LANES]
            tsend[1, NC * chip + k // ng, k % ng] = blk[:, LANES:]
            pbuf[pl.ds(chip * gpc + k, 1), :] = jnp.sum(blk * crow, axis=0, keepdims=True)

        @pl.when(i == 0)
        def _():
            pl.semaphore_wait(barrier, NORB - 1 + NAUX - 1)

        @pl.when(i < NX - 1)
        def _():
            for hh in range(NC):
                t_copy(0, NC * chip + hh, me).start()
        return 0

    lax.fori_loop(0, NX, t_chunk, 0)
    for sp in range(2):
        t_copy(sp, partner, me).start()
        share_own(sp).start()

    ngrp = NORB * ng
    nrow = ngrp // 8
    lane = iota((8, LANES), 1)
    gpart = jnp.zeros((8, LANES), F32)
    for r in range(nrow):
        pa = pbuf[8 * r:8 * r + 8, 0:LANES]
        pb = pbuf[8 * r:8 * r + 8, LANES:2 * LANES]
        for j in range(PACK):
            part = (jnp.where((lane >= na * j) & (lane < na * (j + 1)), pa, 0.0)
                    + jnp.where((lane >= nb * j) & (lane < nb * (j + 1)), pb, 0.0))
            gpart = jnp.where(lane == PACK * r + j, jnp.sum(part, axis=1, keepdims=True), gpart)
    gsend[...] = gpart

    def g_copy(dest, src):
        return remote(gsend, grecv.at[src], gs_sem.at[dest], gr_sem.at[src], orb_dev(dest))

    for o in range(1, NORB):
        g_copy((me + o) % NORB, me).start()
    grecv[me] = gpart
    for dest in far:
        t_copy(1, dest, me).start()
    for g in range(ng):
        for dest in near:
            t_copy(1, dest, me, g).start()
    for sp in range(2):
        trecv[sp, :, rows_of(me), 0:LANES] = tsend[sp, me]
        trecv[sp, :, rows_of(me), LANES:2 * LANES] = tsend[sp, partner]

    def pass_on(sp, sources, g=None):
        for src in sources:
            t_copy(sp, src, src, g).wait_recv()
            share(sp, src, g).start()

    def shared(sp, sources, g=None):
        for src in sources:
            share(sp, src, g).wait_recv()

    def j_copy(dest, src):
        return remote(jsend.at[dest], jrecv.at[src], js_sem.at[dest], jr_sem.at[src], (sysi, dest, me))

    def p1_copy(sp, d):
        q, dev = first_peer(d)
        return remote(kbuf.at[sp, q], r1.at[sp, d - 1], s1_sem.at[sp, d - 1], r1_sem.at[sp, d - 1], dev)

    def p2_copy(sp, d):
        q, dev = second_peer(d)
        return remote(s2.at[sp, q], r2.at[sp, d - 1], s2_sem.at[sp, d - 1], r2_sem.at[sp, d - 1], dev)

    def p3_copy(sp, k):
        return remote(s3.at[sp, k // NC], r3.at[sp, xi], s3_sem.at[sp, k], r3_sem.at[sp, xi],
                      orb_dev(NX * hi + k))

    def p3_wait(sp, x):
        return remote(s3.at[sp, 0], r3.at[sp, x], s3_sem.at[sp, 0], r3_sem.at[sp, x],
                      orb_dev(NC * x + xi // NC))

    def coulomb():
        for o in range(1, NORB):
            src = (me + o) % NORB
            g_copy(src, src).wait_recv()
        gsum = grecv[0]
        for s in range(1, NORB):
            gsum = gsum + grecv[s]
        for r in range(nrow):
            for j in range(PACK):
                c = PACK * r + j
                gam[c * 8:c * 8 + 8, :] = jnp.broadcast_to(gsum[:, c:c + 1], (8, LANES))

        nblk = pl.cdiv(nbas, LANES)
        ends = [(k * LANES, min(nbas, (k + 1) * LANES)) for k in range(nblk)]

        def add(g, acc):
            r, row = g // 8, g % 8
            for j in range(PACK):
                w = gam[pl.ds((PACK * r + j) * 8 + row, 1), :]
                acc = tuple(a + bbuf[g, j, :, lo:hi_] * w[:, :hi_ - lo] for a, (lo, hi_) in zip(acc, ends))
            return acc

        jmat = lax.fori_loop(0, ngrp, add, tuple(jnp.zeros((ml, hi_ - lo), F32) for lo, hi_ in ends))
        for a, (lo, hi_) in zip(jmat, ends):
            jpad[0:ml, lo:hi_] = a
        jt = jpad[...].T
        for a in range(NAUX):
            jsend[a, 0:cols, :] = jt[a * cols:(a + 1) * cols]
        for k in range(1, NAUX):
            j_copy((aux + k) % NAUX, aux).start()
        jrecv[aux] = jsend[aux]

    def k_step(sp, g):
        for h in range(NC):
            @pl.when(hi == h)
            def _():
                for a in range(NZ * NY):
                    at = a if h == 0 else (a % NY) * NZ + a // NY
                    base = (a // 2) * SLOT + (a % 2) * cols
                    tlhs[at * cols:(at + 1) * cols, :] = trecv[sp, g, base:base + cols, :]
        rhs = pl.ds(pl.multiple_of(WIDE * hi, WIDE), WIDE)
        prod = dot_nt(tlhs[...], trecv[sp, g, rhs, :]).reshape(NZ, NY * cols, WIDE)
        kbuf[sp] = kbuf[sp] + prod

    def k_send(sp):
        for d in (2, 1, 3):
            p1_copy(sp, d).start()

    def stage2(sp):
        for d in (1, 3, 2):
            p1_copy(sp, d).wait_recv()
        tot = ((kbuf[sp, p_idx] + r1[sp, 0]) + r1[sp, 1]) + r1[sp, 2]
        for s in range(NY):
            s2[sp, s, 0:cols, :] = tot[s * cols:(s + 1) * cols]
        for d in (2, 1, 3):
            p2_copy(sp, d).start()

    def stage3(sp):
        for d in (1, 3, 2):
            p2_copy(sp, d).wait_recv()
        tot = ((s2[sp, s_idx] + r2[sp, 0]) + r2[sp, 1]) + r2[sp, 2]
        for x in range(NX // NC):
            s3[sp, x] = tot[:, x * LANES:(x + 1) * LANES]
        for k in range(NX):
            @pl.when(NX * hi + k != me)
            def _():
                p3_copy(sp, k).start()

            @pl.when(NX * hi + k == me)
            def _():
                r3[sp, xi] = s3[sp, k // NC]

    def finish(sp, jtot):
        for x in range(NX):
            @pl.when(NC * x + xi // NC != me)
            def _():
                p3_wait(sp, x).wait_recv()
        tot = ((r3[sp, 0] + r3[sp, 1]) + r3[sp, 2]) + r3[sp, 3]
        half = jnp.where(hi == 0, tot[:, :SLOT], tot[:, SLOT:])
        o_ref[sp] = jtot[:cols, :ml] - half[:cols, :ml]

    kbuf[...] = jnp.zeros(kbuf.shape, F32)
    for sp in range(2):
        t_copy(sp, partner, partner).wait_recv()
    pass_on(0, far)
    pass_on(0, near)
    coulomb()
    shared(0, far + near + [partner])

    def alpha_step(g, _):
        k_step(0, g)
        return 0

    lax.fori_loop(0, ng, alpha_step, 0)
    k_send(0)
    pass_on(1, far)
    shared(1, far + [partner])
    pass_on(1, near, 0)

    def beta_step(g, _):
        @pl.when(g < ng - 1)
        def _():
            pass_on(1, near, g + 1)
        shared(1, near, g)
        k_step(1, g)
        return 0

    lax.fori_loop(0, ng, beta_step, 0)
    k_send(1)
    stage2(0)
    stage2(1)
    for k in range(1, NAUX):
        src = (aux + k) % NAUX
        j_copy(src, src).wait_recv()
    jtot = jrecv[0]
    for a in range(1, NAUX):
        jtot = jtot + jrecv[a]
    stage3(0)
    stage3(1)
    finish(0, jtot)
    finish(1, jtot)

    for sp in range(2):
        for g in (range(ng) if sp else (None,)):
            for dest in near:
                t_copy(sp, dest, me, g).wait_send()
                share(sp, dest, g).wait_send()
        for dest in far:
            t_copy(sp, dest, me).wait_send()
            share(sp, dest).wait_send()
        t_copy(sp, partner, me).wait_send()
        share_own(sp).wait_send()
        for d in range(1, NZ):
            p1_copy(sp, d).wait_send()
            p2_copy(sp, d).wait_send()
        for k in range(NX):
            @pl.when(NX * hi + k != me)
            def _():
                p3_copy(sp, k).wait_send()
    for o in range(1, NORB):
        g_copy((me + o) % NORB, me).wait_send()
    for k in range(1, NAUX):
        j_copy((aux + k) % NAUX, aux).wait_send()


def solution(mesh):
    def local_build(b_local, c_alpha, c_beta):
        q_loc, ml, nbas = b_local.shape
        na, nb = c_alpha.shape[1], c_beta.shape[1]
        ng = q_loc // (PACK * NORB)
        b4 = b_local.reshape(q_loc // PACK, PACK, ml, nbas)
        width = NORB * SLOT
        cols = nbas // (NZ * NY)
        dma = pltpu.SemaphoreType.DMA
        vmem = pl.BlockSpec(memory_space=pltpu.VMEM)
        out = pl.pallas_call(
            functools.partial(kernel, (ng, ml, nbas, na, nb)),
            out_shape=jax.ShapeDtypeStruct((2, cols, ml), F32),
            in_specs=[pl.BlockSpec(memory_space=pl.ANY)] * 3,
            out_specs=vmem,
            scratch_shapes=[
                pltpu.VMEM(b4.shape, F32),
                pltpu.VMEM((na, nbas), F32),
                pltpu.VMEM((nb, nbas), F32),
                pltpu.VMEM((PACK, 2 * LANES, nbas), F32),
                pltpu.VMEM((2, NORB, ng, ml, LANES), F32),
                pltpu.VMEM((2, ng, width, NC * LANES), F32),
                pltpu.VMEM((nbas, NC * LANES), F32),
                pltpu.VMEM((q_loc // PACK, 2 * LANES), F32),
                pltpu.VMEM((8, LANES), F32),
                pltpu.VMEM((NORB, 8, LANES), F32),
                pltpu.VMEM((q_loc, LANES), F32),
                pltpu.VMEM((LANES, width), F32),
                pltpu.VMEM((NAUX, HALF, LANES), F32),
                pltpu.VMEM((NAUX, HALF, LANES), F32),
                pltpu.VMEM((2, NZ, NY * cols, WIDE), F32),
                pltpu.VMEM((2, NZ - 1, NY * cols, WIDE), F32),
                pltpu.VMEM((2, NY, HALF, WIDE), F32),
                pltpu.VMEM((2, NZ - 1, HALF, WIDE), F32),
                pltpu.VMEM((2, NX // NC, HALF, LANES), F32),
                pltpu.VMEM((2, NX, HALF, LANES), F32),
                dma((NX,)), dma((2,)), dma((2, NORB, ng)), dma((2, NORB, ng)),
                dma((2, NORB, ng)), dma((2, NORB, ng)), dma((NORB,)), dma((NORB,)), dma((NAUX,)), dma((NAUX,)),
                dma((2, NZ - 1)), dma((2, NZ - 1)), dma((2, NZ - 1)), dma((2, NZ - 1)),
                dma((2, NX)), dma((2, NX)),
            ],
            compiler_params=pltpu.CompilerParams(
                collective_id=0, has_side_effects=True, vmem_limit_bytes=60 * 1024 * 1024),
        )(b4, c_alpha.T, c_beta.T)
        return out[0].T, out[1].T

    spec_b = P(('sys', 'aux'), 'orb', None)
    spec_c = P('sys', None)
    spec_g = P(('sys', 'orb'), 'aux')
    return jax.shard_map(local_build, mesh=mesh, in_specs=(spec_b, spec_c, spec_c), out_specs=(spec_g, spec_g), check_vma=False)
```
